32 devices in a mesh: section: 4 (over y, x), dp: 8 (over z, core).
Axes of the slice: x: 2, y: 2, z: 4, core: 2. Of those that a mesh axis runs over, the one named last changes fastest.
Arguments:
- buffer: bfloat16 [4, 64, 2048], P('section', 'dp'), may hold values from -6 to 6
- gate_weight: bfloat16 [4, 2, 2048, 8192], P('section', None, None, 'dp'), may hold values from -0.125 to 0.125
- up_weight: bfloat16 [4, 2, 2048, 8192], P('section', None, None, 'dp'), may hold values from -0.125 to 0.125
- down_weight: bfloat16 [4, 2, 8192, 2048], P('section', None, 'dp'), may hold values from -0.09375 to 0.09375
- norm_gain: float32 [4, 2, 2048], P('section'), may hold values from 0.1 to 1.9
- repeat_index: int32 [2, 4], P(None, 'section'), may hold values from 0 to 1
Outputs:
- final_buffer: bfloat16 [4, 64, 2048], P('section', 'dp')
The draws below stay inside these ranges and needn't reach their ends.
Inputs may be any that keep to these rules, and one draw needn't show every extreme that they name: `repeat_index`: the layer each section applies, one of its 2.
All inputs are finite; a program needn't handle non-finite values.
Results may differ from the reference program's by a relative error of at most 0.01.
Values may be sent and summed in bfloat16 or wider, within the bound.
A program may use at most 128 MiB of HBM per device.

```python
import jax
import jax.numpy as jnp
from jax import lax

D = 2048
FF = 8192
REPEATS = 2
TICKS = 2
SECTIONS = 4
TOKENS = 64


def with_ends(drawn, stream_key, least, largest):
    dims = drawn.shape
    place = [jax.random.randint(jax.random.fold_in(stream_key, axis), (), 0, dims[axis]) for axis in range(len(dims))]
    drawn = drawn.at[tuple(place)].set(least)
    longest = dims.index(max(dims))
    place[longest] = (place[longest] + 1) % dims[longest]
    return drawn.at[tuple(place)].set(largest)


def levels(own_key, extent, split, least, top_value):
    level, own = 1.0, jax.random.fold_in(own_key, 6)
    for axis_at, shards_of in split:
        heights = jnp.exp(jax.random.uniform(jax.random.fold_in(own, axis_at), (shards_of,), jnp.float32, least / len(split), top_value / len(split)))
        level = level * jnp.repeat(heights, extent[axis_at] // shards_of).reshape([-1 if axis == axis_at else 1 for axis in range(len(extent))])
    return level


def noise(stream_key, dims, scale, most, split=(), kind=jnp.bfloat16):
    result = scale * jax.random.normal(stream_key, dims, jnp.float32)
    if split:
        result = result * levels(stream_key, dims, split, -0.22, 0.18)
    return jnp.clip(result, -most, most).astype(kind)


def setup_inputs(seed: int = 0) -> dict:
    key_of = jax.random.split(jax.random.key(seed), 7)
    buffer = noise(key_of[0], (SECTIONS, TOKENS, D), 1.0, 6.0, ((0, 4), (1, 8)))
    gate_weight = noise(key_of[1], (SECTIONS, REPEATS, D, FF), D ** -0.5, 0.125, ((0, 4), (3, 8)))
    up_weight = noise(key_of[2], (SECTIONS, REPEATS, D, FF), D ** -0.5, 0.125, ((0, 4), (3, 8)))
    down_weight = noise(key_of[3], (SECTIONS, REPEATS, FF, D), (FF // 2) ** -0.5, 0.09375, ((0, 4), (2, 8)))
    norm_gain = jnp.clip(1.0 + 0.18 * jax.random.normal(key_of[4], (SECTIONS, REPEATS, D), jnp.float32), 0.1, 1.9)
    repeat_index = with_ends(jax.random.randint(key_of[5], (TICKS, SECTIONS), 0, REPEATS), jax.random.fold_in(key_of[5], 1), 0, REPEATS - 1).astype(jnp.int32)
    return dict(buffer=buffer, gate_weight=gate_weight, up_weight=up_weight, down_weight=down_weight, norm_gain=norm_gain, repeat_index=repeat_index)


epsilon = 0.5

def apply_layer(tokens, gain_row, gate_slab, up_slab, down_slab):
    widened = tokens.astype(jnp.float32)
    squares = lax.optimization_barrier(jnp.mean(widened * widened, axis=-1, keepdims=True))
    normed = (widened * lax.rsqrt(squares + epsilon) * gain_row[None, :]).astype(jnp.bfloat16)
    gate_value = jnp.dot(normed, gate_slab, preferred_element_type=jnp.float32)
    up_value = jnp.dot(normed, up_slab, preferred_element_type=jnp.float32)
    hidden = (jax.nn.silu(gate_value) * up_value).astype(jnp.bfloat16)
    output = jnp.dot(hidden, down_slab, preferred_element_type=jnp.float32)
    return (widened + output).astype(jnp.bfloat16)

def reference(buffer, gate_weight, up_weight, down_weight, norm_gain, repeat_index):
    current = buffer
    for tick_index in range(TICKS):

        def advance(section_index):
            chosen = repeat_index[tick_index, section_index]
            return apply_layer(current[section_index], norm_gain[section_index, chosen], gate_weight[section_index, chosen], up_weight[section_index, chosen], down_weight[section_index, chosen])
        advanced = lax.map(advance, jnp.arange(SECTIONS, dtype=jnp.int32))
        current = jnp.roll(advanced, 1, axis=0)
    return current
```

```python
import functools

import jax
import jax.numpy as jnp
from jax import lax
from jax.experimental import pallas as pl
from jax.experimental.pallas import tpu as pltpu
from jax.sharding import PartitionSpec as P

MESH = pl.DeviceIdType.MESH
EPSILON = 0.5
GATE_COLUMNS = 256
DOWN_CHUNKS = 4


def flipped(value, mask):
    bit = 1
    while bit <= mask:
        if mask & bit:
            value = value + bit - 2 * bit * (lax.div(value, bit) % 2)
        bit *= 2
    return value


def relay(dims, index_ref, buffer_ref, gain_ref, gate_hbm, up_hbm, down_hbm, out_ref, *scratch):
    ns, nd, ticks, rows, width, gate_chunks, gate_cols, down_chunks, down_cols = dims
    nz = nd // 2
    scratch = list(scratch)
    gates = [scratch.pop(0) for _ in range(gate_chunks)]
    ups = [scratch.pop(0) for _ in range(gate_chunks)]
    downs = [scratch.pop(0) for _ in range(down_chunks)]
    (blocks, normed, hidden, partial, paired, summed, landed, advanced,
     gate_sem, up_sem, down_sem, spread_send, forward_send, block_recv,
     pair_send, pair_recv, row_send, row_recv, shift_send, shift_recv) = scratch

    s = lax.axis_index("section")
    d = lax.axis_index("dp")
    z = lax.div(d, 2)
    core = lax.rem(d, 2)
    other = z * 2 + 1 - core
    after = lax.rem(s + 1, ns)
    before = lax.rem(s + ns - 1, ns)

    def dev(section, position):
        return {"section": section, "dp": position}

    def at(zz):
        return zz * 2 + core

    loads = []
    for i in range(gate_chunks):
        cols = pl.ds(i * gate_cols, gate_cols)
        loads.append(pltpu.make_async_copy(gate_hbm.at[0, :, :, cols], gates[i], gate_sem.at[i]))
        loads.append(pltpu.make_async_copy(up_hbm.at[0, :, :, cols], ups[i], up_sem.at[i]))
    for c in range(down_chunks):
        cols = pl.ds(c * down_cols, down_cols)
        loads.append(pltpu.make_async_copy(down_hbm.at[0, :, :, cols], downs[c], down_sem.at[c]))
    for load in loads:
        load.start()

    barrier = pltpu.get_barrier_semaphore()
    pl.semaphore_signal(barrier, inc=1, device_id=dev(s, other), device_id_type=MESH)
    for j in range(1, nz):
        pl.semaphore_signal(barrier, inc=1, device_id=dev(s, at(flipped(z, j))), device_id_type=MESH)
    for j in range(nz):
        zz = flipped(z, j)
        pl.semaphore_signal(barrier, inc=1, device_id=dev(after, at(zz)), device_id_type=MESH)
        pl.semaphore_signal(barrier, inc=1, device_id=dev(before, at(zz)), device_id_type=MESH)
    pl.semaphore_wait(barrier, 3 * nz)

    sent = []

    def send(src, dst, send_sem, recv_sem, device):
        copy = pltpu.make_async_remote_copy(
            src_ref=src, dst_ref=dst, send_sem=send_sem, recv_sem=recv_sem,
            device_id=device, device_id_type=MESH,
        )
        copy.start()
        sent.append(copy)

    def arrived(dst, recv_sem):
        pltpu.make_async_remote_copy(
            src_ref=dst, dst_ref=dst, send_sem=shift_send, recv_sem=recv_sem,
            device_id=dev(s, other), device_id_type=MESH,
        ).wait_recv()

    for t in range(ticks):
        layer = index_ref[t, 0]
        if t == 0:
            for j in reversed(range(1, nz)):
                send(buffer_ref.at[0], blocks.at[t, d], spread_send.at[t, j], block_recv.at[t, d],
                     dev(s, at(flipped(z, j))))
            send(buffer_ref.at[0], blocks.at[t, d], forward_send.at[t, 0], block_recv.at[t, d], dev(s, other))
            blocks[t, d] = buffer_ref[0]
        else:
            for j in reversed(range(nz)):
                send(advanced.at[t - 1], blocks.at[t, d], spread_send.at[t, j], block_recv.at[t, d],
                     dev(after, at(flipped(z, j))))
        for j in range(nz):
            slot = at(flipped(z, j))
            if t > 0 or j > 0:
                arrived(blocks.at[t, slot], block_recv.at[t, slot])
                send(blocks.at[t, slot], blocks.at[t, slot], forward_send.at[t, j], block_recv.at[t, slot],
                     dev(s, other))
        gain = gain_ref[0, pl.ds(layer, 1), :]
        for j in range(nz):
            zz = flipped(z, j)
            slot = zz * 2 + 1 - core
            arrived(blocks.at[t, slot], block_recv.at[t, slot])
            value = jnp.concatenate(
                [blocks[t, zz * 2].astype(jnp.float32), blocks[t, zz * 2 + 1].astype(jnp.float32)], axis=0
            )
            squares = jnp.mean(value * value, axis=-1, keepdims=True)
            normed[zz] = (value * lax.rsqrt(squares + EPSILON) * gain).astype(jnp.bfloat16)

        for i in range(gate_chunks):
            if t == 0:
                loads[2 * i].wait()
                loads[2 * i + 1].wait()
            tokens = normed[...].reshape(nd * rows, width)
            gate = jnp.dot(tokens, gates[i][layer], preferred_element_type=jnp.float32)
            up = jnp.dot(tokens, ups[i][layer], preferred_element_type=jnp.float32)
            hidden[:, i * gate_cols:(i + 1) * gate_cols] = (
                gate / (1.0 + jnp.exp(-gate)) * up
            ).astype(jnp.bfloat16)

        def scatter(c):
            arrived(paired.at[t, c], pair_recv.at[t, c])
            summed[t, c] = (partial[t, c, core] + paired[t, c]).astype(jnp.bfloat16)
            for j in reversed(range(1, nz)):
                zz = flipped(z, j)
                send(summed.at[t, c, zz], landed.at[t, c, z], row_send.at[t, c, j], row_recv.at[t, c, z],
                     dev(s, at(zz)))

        for c in range(down_chunks):
            if t == 0:
                loads[2 * gate_chunks + c].wait()
            part = jnp.dot(hidden[...], downs[c][layer], preferred_element_type=jnp.float32)
            part = part.reshape(nz, 2, rows, down_cols)
            partial[t, c, 0] = part[:, 0]
            partial[t, c, 1] = part[:, 1]
            send(partial.at[t, c, 1 - core], paired.at[t, c], pair_send.at[t, c], pair_recv.at[t, c],
                 dev(s, other))
            if c > 0:
                scatter(c - 1)
        scatter(down_chunks - 1)

        for c in range(down_chunks):
            total = partial[t, c, core, z] + paired[t, c, z]
            for j in range(1, nz):
                zz = flipped(z, j)
                arrived(landed.at[t, c, zz], row_recv.at[t, c, zz])
                total = total + landed[t, c, zz].astype(jnp.float32)
            cols = slice(c * down_cols, (c + 1) * down_cols)
            advanced[t, :, cols] = (blocks[t, d, :, cols].astype(jnp.float32) + total).astype(jnp.bfloat16)

    send(advanced.at[ticks - 1], out_ref.at[0], shift_send, shift_recv, dev(after, d))
    arrived(out_ref.at[0], shift_recv)
    for copy in sent:
        copy.wait_send()


def on_device(buffer, gate_weight, up_weight, down_weight, norm_gain, repeat_index):
    ns, nd = lax.axis_size("section"), lax.axis_size("dp")
    ticks = repeat_index.shape[0]
    _, rows, width = buffer.shape
    layers, units = gate_weight.shape[1], gate_weight.shape[3]
    nz = nd // 2
    gate_cols = min(GATE_COLUMNS, units)
    gate_chunks = units // gate_cols
    down_chunks = DOWN_CHUNKS
    down_cols = width // down_chunks
    dims = (ns, nd, ticks, rows, width, gate_chunks, gate_cols, down_chunks, down_cols)
    bf16, f32, DMA = jnp.bfloat16, jnp.float32, pltpu.SemaphoreType.DMA
    scratch = (
        [pltpu.VMEM((layers, width, gate_cols), bf16)] * (2 * gate_chunks)
        + [pltpu.VMEM((layers, units, down_cols), bf16)] * down_chunks
        + [
            pltpu.VMEM((ticks, nd, rows, width), bf16),
            pltpu.VMEM((nz, 2 * rows, width), bf16),
            pltpu.VMEM((nd * rows, units), bf16),
            pltpu.VMEM((ticks, down_chunks, 2, nz, rows, down_cols), f32),
            pltpu.VMEM((ticks, down_chunks, nz, rows, down_cols), f32),
            pltpu.VMEM((ticks, down_chunks, nz, rows, down_cols), bf16),
            pltpu.VMEM((ticks, down_chunks, nz, rows, down_cols), bf16),
            pltpu.VMEM((ticks, rows, width), bf16),
            DMA((gate_chunks,)), DMA((gate_chunks,)), DMA((down_chunks,)),
            DMA((ticks, nz)), DMA((ticks, nz)), DMA((ticks, nd)),
            DMA((ticks, down_chunks)), DMA((ticks, down_chunks)),
            DMA((ticks, down_chunks, nz)), DMA((ticks, down_chunks, nz)),
            DMA, DMA,
        ]
    )
    vmem = pl.BlockSpec(memory_space=pltpu.VMEM)
    smem = pl.BlockSpec(memory_space=pltpu.SMEM)
    hbm = pl.BlockSpec(memory_space=pl.ANY)
    return pl.pallas_call(
        functools.partial(relay, dims),
        out_shape=jax.ShapeDtypeStruct(buffer.shape, buffer.dtype),
        in_specs=[smem, vmem, vmem, hbm, hbm, hbm],
        out_specs=vmem,
        scratch_shapes=scratch,
        compiler_params=pltpu.CompilerParams(
            collective_id=0, has_side_effects=True, vmem_limit_bytes=60_000_000
        ),
    )(repeat_index, buffer, norm_gain, gate_weight, up_weight, down_weight)


def solution(mesh):
    placed = (
        P("section", "dp", None),
        P("section", None, None, "dp"),
        P("section", None, None, "dp"),
        P("section", None, "dp", None),
        P("section", None, None),
        P(None, "section"),
    )
    return jax.shard_map(
        on_device, mesh=mesh, in_specs=placed, out_specs=P("section", "dp", None), check_vma=False
    )
```

```python
import functools

import jax
import jax.numpy as jnp
from jax import lax
from jax.experimental import pallas as pl
from jax.experimental.pallas import tpu as pltpu
from jax.sharding import PartitionSpec as P

MESH = pl.DeviceIdType.MESH
EPSILON = 0.5
GATE_COLUMNS = 512
DOWN_CHUNKS = 2


def flipped(value, mask):
    bit = 1
    while bit <= mask:
        if mask & bit:
            value = value + bit - 2 * bit * (lax.div(value, bit) % 2)
        bit *= 2
    return value


def relay(dims, index_hbm, buffer_ref, gain_ref, gate_hbm, up_hbm, down_hbm, out_ref, *scratch):
    ns, nd, ticks, rows, width, gate_chunks, gate_cols, down_chunks, down_cols = dims
    nz = nd // 2
    scratch = list(scratch)
    gates = [scratch.pop(0) for _ in range(gate_chunks)]
    ups = [scratch.pop(0) for _ in range(gate_chunks)]
    downs = [scratch.pop(0) for _ in range(down_chunks)]
    (blocks, normed, hidden, partial, paired, summed, landed, advanced,
     gate_sem, up_sem, down_sem, spread_send, forward_send, block_recv,
     pair_send, pair_recv, row_send, row_recv, shift_send, shift_recv,
     residual, index_ref, index_sem, ready) = scratch

    s = lax.axis_index("section")
    d = lax.axis_index("dp")
    z = lax.div(d, 2)
    core = lax.rem(d, 2)
    other = z * 2 + 1 - core
    after = lax.rem(s + 1, ns)
    before = lax.rem(s + ns - 1, ns)

    def dev(section, position):
        return {"section": section, "dp": position}

    def at(zz):
        return zz * 2 + core

    index_load = pltpu.make_async_copy(index_hbm, index_ref, index_sem)
    index_load.start()
    loads = []
    for i in range(gate_chunks):
        cols = pl.ds(i * gate_cols, gate_cols)
        loads.append(pltpu.make_async_copy(gate_hbm.at[0, :, :, cols], gates[i], gate_sem.at[i]))
        loads.append(pltpu.make_async_copy(up_hbm.at[0, :, :, cols], ups[i], up_sem.at[i]))
    for c in range(down_chunks):
        cols = pl.ds(c * down_cols, down_cols)
        loads.append(pltpu.make_async_copy(down_hbm.at[0, :, :, cols], downs[c], down_sem.at[c]))
    for load in loads:
        load.start()

    barrier = pltpu.get_barrier_semaphore()
    pl.semaphore_signal(barrier, inc=1, device_id=dev(s, other), device_id_type=MESH)
    for j in range(1, nz):
        pl.semaphore_signal(barrier, inc=1, device_id=dev(s, at(flipped(z, j))), device_id_type=MESH)
    for section in (after, before):
        pl.semaphore_signal(barrier, inc=1, device_id=dev(section, d), device_id_type=MESH)
    pl.semaphore_wait(barrier, nz + 2)
    pl.semaphore_signal(ready, inc=1, device_id=dev(before, d), device_id_type=MESH)

    sent = []

    def send(src, dst, send_sem, recv_sem, device):
        copy = pltpu.make_async_remote_copy(
            src_ref=src, dst_ref=dst, send_sem=send_sem, recv_sem=recv_sem,
            device_id=device, device_id_type=MESH,
        )
        copy.start()
        sent.append(copy)

    def arrived(dst, recv_sem):
        pltpu.make_async_remote_copy(
            src_ref=dst, dst_ref=dst, send_sem=shift_send, recv_sem=recv_sem,
            device_id=dev(s, other), device_id_type=MESH,
        ).wait_recv()

    def await_section():
        pl.semaphore_wait(ready, 1)

    for t in range(ticks):
        last = t == ticks - 1
        if t == 0:
            for j in reversed(range(1, nz)):
                send(buffer_ref.at[0], blocks.at[t, d], spread_send.at[t, j], block_recv.at[t, d],
                     dev(s, at(flipped(z, j))))
            send(buffer_ref.at[0], blocks.at[t, d], forward_send.at[t, 0], block_recv.at[t, d], dev(s, other))
            blocks[t, d] = buffer_ref[0]
        else:
            if t == 1:
                await_section()
            for j in reversed(range(nz)):
                send(advanced.at[t - 1], blocks.at[t, d], spread_send.at[t, j], block_recv.at[t, d],
                     dev(after, at(flipped(z, j))))
        for j in range(nz):
            slot = at(flipped(z, j))
            if t > 0 or j > 0:
                arrived(blocks.at[t, slot], block_recv.at[t, slot])
                send(blocks.at[t, slot], blocks.at[t, slot], forward_send.at[t, j], block_recv.at[t, slot],
                     dev(s, other))
        if last:
            if t == 0:
                await_section()
            kept = buffer_ref.at[0] if t == 0 else blocks.at[t, d]
            send(kept, residual, shift_send, shift_recv, dev(after, d))
        if t == 0:
            index_load.wait()
        layer = index_ref[t, 0]
        gain = gain_ref[0, pl.ds(layer, 1), :]
        for j in range(nz):
            zz = flipped(z, j)
            slot = zz * 2 + 1 - core
            arrived(blocks.at[t, slot], block_recv.at[t, slot])
            value = jnp.concatenate(
                [blocks[t, zz * 2].astype(jnp.float32), blocks[t, zz * 2 + 1].astype(jnp.float32)], axis=0
            )
            squares = jnp.mean(value * value, axis=-1, keepdims=True)
            normed[zz] = (value * lax.rsqrt(squares + EPSILON) * gain).astype(jnp.bfloat16)

        for i in range(gate_chunks):
            if t == 0:
                loads[2 * i].wait()
                loads[2 * i + 1].wait()
            tokens = normed[...].reshape(nd * rows, width)
            gate = jnp.dot(tokens, gates[i][layer], preferred_element_type=jnp.float32)
            up = jnp.dot(tokens, ups[i][layer], preferred_element_type=jnp.float32)
            hidden[:, i * gate_cols:(i + 1) * gate_cols] = (
                gate / (1.0 + jnp.exp(-gate)) * up
            ).astype(jnp.bfloat16)

        def scatter(c):
            arrived(paired.at[t, c], pair_recv.at[t, c])
            summed[t, c] = (partial[t, c, core] + paired[t, c]).astype(jnp.bfloat16)
            for j in reversed(range(0 if last else 1, nz)):
                zz = flipped(z, j)
                send(summed.at[t, c, zz], landed.at[t, c, z], row_send.at[t, c, j], row_recv.at[t, c, z],
                     dev(after if last else s, at(zz)))

        for c in range(down_chunks):
            if t == 0:
                loads[2 * gate_chunks + c].wait()
            part = jnp.dot(hidden[...], downs[c][layer], preferred_element_type=jnp.float32)
            part = part.reshape(nz, 2, rows, down_cols)
            partial[t, c, 0] = part[:, 0]
            partial[t, c, 1] = part[:, 1]
            send(partial.at[t, c, 1 - core], paired.at[t, c], pair_send.at[t, c], pair_recv.at[t, c],
                 dev(s, other))
            if c > 0:
                scatter(c - 1)
        scatter(down_chunks - 1)

        if last:
            arrived(residual, shift_recv)
        for c in range(down_chunks):
            cols = slice(c * down_cols, (c + 1) * down_cols)
            if last:
                total = residual[:, cols].astype(jnp.float32)
            else:
                total = blocks[t, d, :, cols].astype(jnp.float32) + partial[t, c, core, z] + paired[t, c, z]
            for j in range(0 if last else 1, nz):
                zz = flipped(z, j)
                arrived(landed.at[t, c, zz], row_recv.at[t, c, zz])
                total = total + landed[t, c, zz].astype(jnp.float32)
            if last:
                out_ref[0, :, cols] = total.astype(jnp.bfloat16)
            else:
                advanced[t, :, cols] = total.astype(jnp.bfloat16)

    for copy in sent:
        copy.wait_send()


def on_device(buffer, gate_weight, up_weight, down_weight, norm_gain, repeat_index):
    ns, nd = lax.axis_size("section"), lax.axis_size("dp")
    ticks = repeat_index.shape[0]
    _, rows, width = buffer.shape
    layers, units = gate_weight.shape[1], gate_weight.shape[3]
    nz = nd // 2
    gate_cols = min(GATE_COLUMNS, units)
    gate_chunks = units // gate_cols
    down_chunks = DOWN_CHUNKS
    down_cols = width // down_chunks
    dims = (ns, nd, ticks, rows, width, gate_chunks, gate_cols, down_chunks, down_cols)
    bf16, f32, DMA = jnp.bfloat16, jnp.float32, pltpu.SemaphoreType.DMA
    scratch = (
        [pltpu.VMEM((layers, width, gate_cols), bf16)] * (2 * gate_chunks)
        + [pltpu.VMEM((layers, units, down_cols), bf16)] * down_chunks
        + [
            pltpu.VMEM((ticks, nd, rows, width), bf16),
            pltpu.VMEM((nz, 2 * rows, width), bf16),
            pltpu.VMEM((nd * rows, units), bf16),
            pltpu.VMEM((ticks, down_chunks, 2, nz, rows, down_cols), f32),
            pltpu.VMEM((ticks, down_chunks, nz, rows, down_cols), f32),
            pltpu.VMEM((ticks, down_chunks, nz, rows, down_cols), bf16),
            pltpu.VMEM((ticks, down_chunks, nz, rows, down_cols), bf16),
            pltpu.VMEM((ticks, rows, width), bf16),
            DMA((gate_chunks,)), DMA((gate_chunks,)), DMA((down_chunks,)),
            DMA((ticks, nz)), DMA((ticks, nz)), DMA((ticks, nd)),
            DMA((ticks, down_chunks)), DMA((ticks, down_chunks)),
            DMA((ticks, down_chunks, nz)), DMA((ticks, down_chunks, nz)),
            DMA, DMA,
            pltpu.VMEM((rows, width), bf16), pltpu.SMEM((ticks, 1), jnp.int32), DMA,
            pltpu.SemaphoreType.REGULAR,
        ]
    )
    vmem = pl.BlockSpec(memory_space=pltpu.VMEM)
    hbm = pl.BlockSpec(memory_space=pl.ANY)
    return pl.pallas_call(
        functools.partial(relay, dims),
        out_shape=jax.ShapeDtypeStruct(buffer.shape, buffer.dtype),
        in_specs=[hbm, vmem, vmem, hbm, hbm, hbm],
        out_specs=vmem,
        scratch_shapes=scratch,
        compiler_params=pltpu.CompilerParams(
            collective_id=0, has_side_effects=True, vmem_limit_bytes=60_000_000
        ),
    )(repeat_index, buffer, norm_gain, gate_weight, up_weight, down_weight)


def solution(mesh):
    placed = (
        P("section", "dp", None),
        P("section", None, None, "dp"),
        P("section", None, None, "dp"),
        P("section", None, "dp", None),
        P("section", None, None),
        P(None, "section"),
    )
    return jax.shard_map(
        on_device, mesh=mesh, in_specs=placed, out_specs=P("section", "dp", None), check_vma=False
    )
```
